16 devices in a mesh: dp: 4 (over z, y), tp: 4 (over x, core).
Axes of the slice: x: 2, y: 2, z: 2, core: 2. Of those that a mesh axis runs over, the one named last changes fastest.
Arguments:
- tokens: int32 [4, 2048], P('dp')
- emb_table: bfloat16 [65536, 3072], P('tp')
- w_norm: float32 [3072], replicated
- dy_norm: bfloat16 [4, 2048, 3072], P('dp', 'tp')
- dy_resid: bfloat16 [4, 2048, 3072], P('dp', 'tp')
Outputs:
- output 1: bfloat16 [4, 2048, 3072], P('dp', 'tp')
- output 2: bfloat16 [4, 2048, 3072], P('dp', 'tp')
- output 3: float32 [65536, 3072], P(('tp', 'dp'))
- output 4: float32 [3072], replicated
All inputs are finite; a program needn't handle non-finite values.
Results may differ from the reference program's by a relative error of at most 0.00840549.
Values sent between devices are 32-bit elements.
A program may use at most 1 GiB of HBM per device.

```python
import jax
import jax.numpy as jnp
from jax import lax

VOCAB_ROWS = 65536
MODEL_DIM = 3072
NUM_SEQS = 4
SEQ_LEN = 2048
NORM_EPS = 1e-6
LOG_VOCAB = (VOCAB_ROWS - 1).bit_length()


def draw_tokens(key):
    k_level, k_ident, k_pick, k_flat = jax.random.split(key, 4)
    tok_shape = (NUM_SEQS, SEQ_LEN)
    zipf_level = jax.random.randint(k_level, tok_shape, 0, LOG_VOCAB + 1, dtype=jnp.int32)
    level_top = jnp.minimum(jnp.left_shift(jnp.ones(tok_shape, jnp.int32), zipf_level), VOCAB_ROWS)
    zipf_ids = jax.random.randint(k_ident, tok_shape, 0, level_top, dtype=jnp.int32)
    flat_ids = jax.random.randint(k_flat, tok_shape, 0, VOCAB_ROWS, dtype=jnp.int32)
    mix_pick = jax.random.randint(k_pick, tok_shape, 0, 4, dtype=jnp.int32)
    token_ids = jnp.where(mix_pick == 0, flat_ids, zipf_ids)
    return token_ids.at[0, 0].set(VOCAB_ROWS - 1)


def setup_inputs(seed: int = 0) -> dict:
    k_tok, k_tab, k_gain, k_norm, k_resid = jax.random.split(jax.random.key(seed), 5)
    tokens = draw_tokens(k_tok)
    emb_table = (jax.random.normal(k_tab, (VOCAB_ROWS, MODEL_DIM), jnp.float32) * MODEL_DIM ** -0.5).astype(jnp.bfloat16)
    w_norm = 0.6 * jax.random.normal(k_gain, (MODEL_DIM,), jnp.float32)
    dy_norm = jax.random.normal(k_norm, (NUM_SEQS, SEQ_LEN, MODEL_DIM), jnp.float32).astype(jnp.bfloat16)
    dy_resid = jax.random.normal(k_resid, (NUM_SEQS, SEQ_LEN, MODEL_DIM), jnp.float32).astype(jnp.bfloat16)
    return {"tokens": tokens, "emb_table": emb_table, "w_norm": w_norm, "dy_norm": dy_norm, "dy_resid": dy_resid}


def reference(tokens, emb_table, w_norm, dy_norm, dy_resid):
    emb_scale = jnp.asarray(MODEL_DIM ** 0.5, jnp.bfloat16)
    x_emb = emb_table[tokens] * emb_scale
    x_float = x_emb.astype(jnp.float32)
    inv_rms = lax.rsqrt(jnp.mean(x_float * x_float, axis=-1, keepdims=True) + NORM_EPS)
    x_hat = x_float * inv_rms
    norm_gain = 1.0 + w_norm
    y_norm = (x_hat * norm_gain).astype(jnp.bfloat16)
    dy_float = dy_norm.astype(jnp.float32)
    dx_hat = dy_float * norm_gain
    tok_grad = dy_resid.astype(jnp.float32) + inv_rms * (dx_hat - x_hat * jnp.mean(dx_hat * x_hat, axis=-1, keepdims=True))
    w_grad = jnp.sum(dy_float * x_hat, axis=(0, 1))
    emb_grad = jax.ops.segment_sum(tok_grad.reshape(-1, MODEL_DIM), tokens.reshape(-1), num_segments=VOCAB_ROWS) * emb_scale.astype(jnp.float32)
    return x_emb, y_norm, emb_grad, w_grad
```

```python
import functools
import math
import jax
import jax.numpy as jnp
import numpy as np
from jax import lax
from jax.sharding import PartitionSpec as P
from jax.experimental import pallas as pl
from jax.experimental.pallas import tpu as pltpu

NORM_EPS = 1e-6
MESH = pl.DeviceIdType.MESH
NDEV = 16
OWN_ROWS = 4096
CAPS = (1536, 576, 368, 368) + (288,) * 4 + (224,) * 8
HALF = tuple(c // 2 for c in CAPS)
HBASE = tuple(sum(HALF[:i]) for i in range(NDEV))
HTOT = sum(HALF)
CAPMAX = max(CAPS)
FWD_CHUNKS = 2
TILE = 128


def coords():
    dp, tp = lax.axis_index("dp"), lax.axis_index("tp")
    return dp // 2, dp % 2, tp // 2, tp % 2


def peer(z, y, x, c, k):
    pz, py, px = (z + k // 4) % 2, (y + (k // 2) % 2) % 2, (x + k % 2) % 2
    dp, tp = pz * 2 + py, px * 2 + c
    return dp, tp, dp * 2 + px


def columns_kernel(g_ref, out_ref, stage, send, recv, fsend, frecv, lsem):
    z, y, x, c = coords()
    dp, tp = z * 2 + y, x * 2 + c
    q = dp * 2 + x
    cols = out_ref.shape[2]
    partner = (dp, x * 2 + (1 - c))
    barrier = pltpu.get_barrier_semaphore()
    for k in range(1, 8):
        pdp, ptp, _ = peer(z, y, x, c, k)
        pl.semaphore_signal(barrier, inc=1, device_id=(pdp, ptp), device_id_type=MESH)
    pl.semaphore_signal(barrier, inc=1, device_id=partner, device_id_type=MESH)
    pl.semaphore_wait(barrier, 8)

    def block(qq):
        return g_ref.at[:, pl.ds(pl.multiple_of(qq * cols, 128), cols)]

    sends = []
    for k in (7, 3, 5, 6, 1, 2, 4):
        pdp, ptp, pq = peer(z, y, x, c, k)
        cp = pltpu.make_async_remote_copy(
            src_ref=block(pq), dst_ref=out_ref.at[q * 2 + c],
            send_sem=send.at[k], recv_sem=recv.at[k],
            device_id=(pdp, ptp), device_id_type=MESH)
        cp.start()
        sends.append((k, pq, cp))
    fwd = pltpu.make_async_remote_copy(
        src_ref=block(q), dst_ref=out_ref.at[q * 2 + c],
        send_sem=fsend.at[0], recv_sem=frecv.at[0],
        device_id=partner, device_id_type=MESH)
    fwd.start()
    forwards = [fwd]
    cin = pltpu.make_async_copy(block(q), stage, lsem.at[0])
    cin.start()
    cin.wait()
    cout = pltpu.make_async_copy(stage, out_ref.at[q * 2 + c], lsem.at[1])
    cout.start()
    for k, pq, cp in sorted(sends, key=lambda s: bin(s[0]).count("1")):
        cp.wait_recv()
        f = pltpu.make_async_remote_copy(
            src_ref=out_ref.at[pq * 2 + c], dst_ref=out_ref.at[pq * 2 + c],
            send_sem=fsend.at[k], recv_sem=frecv.at[k],
            device_id=partner, device_id_type=MESH)
        f.start()
        forwards.append(f)
    cout.wait()
    for k, pq, cp in sends:
        cp.wait_send()
    for f in forwards:
        f.wait()


def exchange_columns(g):
    rows, width = g.shape
    cols = width // 8
    return pl.pallas_call(
        columns_kernel,
        out_shape=jax.ShapeDtypeStruct((NDEV, rows, cols), g.dtype),
        in_specs=[pl.BlockSpec(memory_space=pl.ANY)],
        out_specs=pl.BlockSpec(memory_space=pl.ANY),
        scratch_shapes=[
            pltpu.VMEM((rows, cols), g.dtype),
            pltpu.SemaphoreType.DMA((8,)),
            pltpu.SemaphoreType.DMA((8,)),
            pltpu.SemaphoreType.DMA((8,)),
            pltpu.SemaphoreType.DMA((8,)),
            pltpu.SemaphoreType.DMA((2,)),
        ],
        compiler_params=pltpu.CompilerParams(collective_id=1, has_side_effects=True),
        name="exchange_columns",
    )(g)


def sum_kernel(rows, tok_rows, work_ref, count_ref, got_ref, acc_ref, acc2):
    acc_ref[...] = jnp.zeros_like(acc_ref)
    acc2[...] = jnp.zeros_like(acc2)
    wsum = got_ref[pl.ds(tok_rows, 8), :]
    for s in range(1, NDEV):
        wsum = wsum + got_ref[pl.ds(s * rows + tok_rows, 8), :]
    n = count_ref[0]

    def add(ref, i):
        w = work_ref[i]
        p = w % 4096
        r = w // 4096
        ref[pl.ds(p, 1), :] += got_ref[pl.ds(r, 1), :]

    def body(i, carry):
        for u in range(4):
            add(acc_ref, i * 8 + 2 * u)
            add(acc2, i * 8 + 2 * u + 1)
        return carry

    lax.fori_loop(0, n // 8, body, 0)

    def tail(i, carry):
        add(acc_ref, i)
        return carry

    lax.fori_loop((n // 8) * 8, n, tail, 0)
    acc_ref[...] += acc2[...]
    acc_ref[pl.ds(HTOT, 8), :] = wsum


def sum_duplicates(work, count, got, tok_rows):
    _, rows, cols = got.shape
    out_rows = HTOT + 8
    return pl.pallas_call(
        functools.partial(sum_kernel, rows, tok_rows),
        grid_spec=pltpu.PrefetchScalarGridSpec(
            num_scalar_prefetch=2, grid=(1,),
            in_specs=[pl.BlockSpec((NDEV * rows, cols), lambda i, *_: (0, 0))],
            out_specs=pl.BlockSpec((out_rows, cols), lambda i, *_: (0, 0)),
            scratch_shapes=[pltpu.VMEM((out_rows, cols), jnp.float32)],
        ),
        out_shape=jax.ShapeDtypeStruct((out_rows, cols), jnp.float32),
        compiler_params=pltpu.CompilerParams(vmem_limit_bytes=60 * 2**20),
        name="sum_duplicates",
    )(work, count, got.reshape(NDEV * rows, cols))


def owners_kernel(acc_ref, got_ref, w_ref, send, recv, wsend, wrecv, lsem):
    z, y, x, c = coords()
    dp, tp = z * 2 + y, x * 2 + c
    q = dp * 2 + x
    me = q * 2 + c
    own = tp * 4 + dp
    cols = acc_ref.shape[1]
    lanes = pl.ds(pl.multiple_of(q * cols, 128), cols)
    barrier = pltpu.get_barrier_semaphore()
    for d in range(NDEV):
        @pl.when(own != d)
        def _():
            pl.semaphore_signal(barrier, inc=1, device_id=(d % 4, d // 4), device_id_type=MESH)
    pl.semaphore_wait(barrier, NDEV - 1)

    def remote(d):
        h = HALF[d]
        return pltpu.make_async_remote_copy(
            src_ref=acc_ref.at[pl.ds(HBASE[d], h), :],
            dst_ref=got_ref.at[pl.ds(pl.multiple_of(c * h, 8), h), lanes],
            send_sem=send.at[d], recv_sem=recv.at[me],
            device_id=(d % 4, d // 4), device_id_type=MESH)

    def local(d):
        h = HALF[d]
        return pltpu.make_async_copy(
            acc_ref.at[pl.ds(HBASE[d], h), :],
            got_ref.at[pl.ds(pl.multiple_of(c * h, 8), h), lanes], lsem.at[0])

    wrow = acc_ref.at[pl.ds(HTOT, 8), :]

    def wcopy(k):
        pdp, ptp, _ = peer(z, y, x, c, k)
        return pltpu.make_async_remote_copy(
            src_ref=wrow, dst_ref=w_ref.at[:, lanes],
            send_sem=wsend.at[k], recv_sem=wrecv.at[k],
            device_id=(pdp, ptp), device_id_type=MESH)

    for k in range(1, 8):
        wcopy(k).start()
    wlocal = pltpu.make_async_copy(wrow, w_ref.at[:, lanes], lsem.at[1])
    wlocal.start()
    for d in range(NDEV):
        @pl.when(own != d)
        def _():
            remote(d).start()

        @pl.when(own == d)
        def _():
            local(d).start()
    for k in range(1, 8):
        wcopy(k).wait()
    wlocal.wait()
    for d in range(NDEV):
        h = HALF[d]

        @pl.when(own == d)
        def _():
            local(d).wait()
            for s in range(NDEV):
                @pl.when(me != s)
                def _():
                    pltpu.make_async_remote_copy(
                        src_ref=acc_ref.at[pl.ds(HBASE[d], h), :],
                        dst_ref=got_ref.at[pl.ds((s % 2) * h, h), pl.ds((s // 2) * cols, cols)],
                        send_sem=send.at[d], recv_sem=recv.at[s],
                        device_id=(s // 4, s % 4), device_id_type=MESH).wait_recv()

        @pl.when(own != d)
        def _():
            remote(d).wait_send()


def send_to_owners(acc):
    cols = acc.shape[1]
    return pl.pallas_call(
        owners_kernel,
        out_shape=(jax.ShapeDtypeStruct((CAPMAX, cols * 8), jnp.float32),
                   jax.ShapeDtypeStruct((8, cols * 8), jnp.float32)),
        in_specs=[pl.BlockSpec(memory_space=pltpu.VMEM)],
        out_specs=(pl.BlockSpec(memory_space=pl.ANY), pl.BlockSpec(memory_space=pl.ANY)),
        scratch_shapes=[
            pltpu.SemaphoreType.DMA((NDEV,)),
            pltpu.SemaphoreType.DMA((NDEV,)),
            pltpu.SemaphoreType.DMA((8,)),
            pltpu.SemaphoreType.DMA((8,)),
            pltpu.SemaphoreType.DMA((2,)),
        ],
        compiler_params=pltpu.CompilerParams(collective_id=2, has_side_effects=True),
        name="send_to_owners",
    )(acc)


def expand_kernel(scale, bounds_ref, ids_ref, got_ref, out_ref):
    t = pl.program_id(0)
    half = bounds_ref[OWN_ROWS // TILE + 1]
    base = bounds_ref[OWN_ROWS // TILE + 2] + t * TILE
    out_ref[...] = jnp.zeros_like(out_ref)

    def body(s, carry):
        r = ids_ref[s] - base
        src = (s % 2) * half + s // 2
        out_ref[pl.ds(r, 1), :] = got_ref[pl.ds(src, 1), :] * scale
        return carry

    lax.fori_loop(bounds_ref[t], bounds_ref[t + 1], body, 0)


def expand(bounds, ids, got, scale):
    width = got.shape[1]
    return pl.pallas_call(
        functools.partial(expand_kernel, scale),
        grid_spec=pltpu.PrefetchScalarGridSpec(
            num_scalar_prefetch=2, grid=(OWN_ROWS // TILE,),
            in_specs=[pl.BlockSpec((CAPMAX, width), lambda i, *_: (0, 0))],
            out_specs=pl.BlockSpec((TILE, width), lambda i, *_: (i, 0)),
        ),
        out_shape=jax.ShapeDtypeStruct((OWN_ROWS, width), jnp.float32),
        compiler_params=pltpu.CompilerParams(vmem_limit_bytes=60 * 2**20),
        name="expand",
    )(bounds, ids, got)


def solution(mesh):
    def plan(all_ids, rows):
        n = all_ids.shape[0]
        dp, tp = lax.axis_index("dp"), lax.axis_index("tp")
        me, core = tp * 4 + dp, tp % 2
        keys = lax.sort(all_ids * n + lax.iota(jnp.int32, n))
        ids, idx = keys // n, keys % n
        first = jnp.concatenate([jnp.ones((1,), jnp.int32), (ids[1:] != ids[:-1]).astype(jnp.int32)])
        slot = jnp.cumsum(first) - 1
        edges = jnp.arange(NDEV + 1, dtype=jnp.int32) * OWN_ROWS
        starts = jnp.sum(jnp.where(ids[None, :] < edges[:, None], first[None, :], 0), axis=1)
        caps = jnp.array(CAPS, jnp.int32)
        overflow = jnp.any(starts[1:] - starts[:-1] > caps)
        owner = ids // OWN_ROWS
        hit = owner[None, :] == jnp.arange(NDEV, dtype=jnp.int32)[:, None]
        offset = jnp.sum(jnp.where(hit, starts[:-1][:, None], 0), axis=0)
        hbase = jnp.sum(jnp.where(hit, jnp.array(HBASE, jnp.int32)[:, None], 0), axis=0)
        local_slot = slot - offset
        pos = jnp.minimum(hbase + local_slot // 2, HTOT - 1)
        mine = local_slot % 2 == core
        src = (idx // 512) * rows + idx % 512
        work = lax.sort(jnp.where(mine, 0, 1 << 26) + src * 4096 + pos)
        count = jnp.sum(mine.astype(jnp.int32)).reshape(1)
        uniq = lax.sort(jnp.where(first == 1, ids, 1 << 20))
        uniq = jnp.concatenate([uniq, jnp.full((CAPMAX,), 1 << 20, jnp.int32)])
        my_start = jnp.sum(jnp.where(jnp.arange(NDEV) == me, starts[:-1], 0))
        my_ids = lax.dynamic_slice(uniq, (my_start,), (CAPMAX,))
        tiles = me * OWN_ROWS + jnp.arange(OWN_ROWS // TILE + 1, dtype=jnp.int32) * TILE
        bounds = jnp.sum(jnp.where(ids[None, :] < tiles[:, None], first[None, :], 0), axis=1) - my_start
        my_half = jnp.sum(jnp.where(jnp.arange(NDEV) == me, jnp.array(HALF, jnp.int32), 0))
        bounds = jnp.concatenate([bounds, my_half[None], (me * OWN_ROWS)[None]]).astype(jnp.int32)
        return overflow, work, count, my_ids, bounds

    def local_step(tokens, emb_table, w_norm, dy_norm, dy_resid):
        shard_rows, model_dim = emb_table.shape
        scale_float = jnp.asarray(math.sqrt(model_dim), jnp.bfloat16).astype(jnp.float32)
        scale_py = float(np.array(math.sqrt(model_dim)).astype(jnp.dtype(jnp.bfloat16)))
        tp = lax.axis_index("tp")
        x, c = tp // 2, tp % 2
        seq = tokens.shape[1]
        part = seq // 4
        local_ids = tokens[0] - tp * shard_rows
        all_ids = lax.all_gather(tokens, "dp", axis=0, tiled=True).reshape(-1)

        def rows_of(px, pc, k):
            n = part // FWD_CHUNKS
            ids = lax.dynamic_slice(local_ids, ((px * 2 + pc) * part + k * n,), (n,))
            owned = (ids >= 0) & (ids < shard_rows)
            got = jnp.take(emb_table, jnp.where(owned, ids, 0), axis=0, mode="clip")
            return jnp.where(owned[:, None], got.astype(jnp.float32) * scale_float, 0.0)

        swap_core = [(t, t ^ 1) for t in range(4)]
        swap_x = [(t, t ^ 2) for t in range(4)]
        pieces = []
        for k in range(FWD_CHUNKS):
            far = lax.ppermute(rows_of(1 - x, 1 - c, k), "tp", swap_core) + rows_of(1 - x, c, k)
            pieces.append(lax.ppermute(far, "tp", swap_x))
        near = [lax.ppermute(rows_of(x, 1 - c, k), "tp", swap_core) + rows_of(x, c, k) for k in range(FWD_CHUNKS)]
        x_emb = jnp.concatenate([n + f for n, f in zip(near, pieces)], axis=0).astype(jnp.bfloat16)[None]

        x_float = x_emb.astype(jnp.float32)
        inv_rms = lax.rsqrt(jnp.mean(x_float * x_float, axis=-1, keepdims=True) + NORM_EPS)
        x_hat = x_float * inv_rms
        norm_gain = 1.0 + w_norm
        y_norm = (x_hat * norm_gain).astype(jnp.bfloat16)
        dy_float = dy_norm.astype(jnp.float32)
        dx_hat = dy_float * norm_gain
        tok_grad = dy_resid.astype(jnp.float32) + inv_rms * (dx_hat - x_hat * jnp.mean(dx_hat * x_hat, axis=-1, keepdims=True))
        w_part = jnp.sum(dy_float * x_hat, axis=(0, 1))
        rows = part + 8
        g_ext = jnp.concatenate([tok_grad[0], jnp.pad(w_part[None], ((0, 7), (0, 0)))], axis=0)

        overflow, work, count, my_ids, bounds = plan(all_ids, rows)
        got = exchange_columns(g_ext)
        acc = sum_duplicates(work, count, got, part)
        sums, w_rows = send_to_owners(acc)

        def dense(_):
            owned = (local_ids >= 0) & (local_ids < shard_rows)
            seq_grad = lax.all_gather(tok_grad, "tp", axis=1, tiled=True)
            drop_ids = jnp.where(owned, local_ids, shard_rows)
            shard_grad = jax.ops.segment_sum(seq_grad.reshape(-1, model_dim), drop_ids, num_segments=shard_rows, mode="drop") * scale_float
            return lax.psum_scatter(shard_grad, "dp", scatter_dimension=0, tiled=True)

        def sparse(_):
            return expand(bounds, my_ids, sums, scale_py)

        emb_grad = lax.cond(overflow, dense, sparse, 0)
        return x_emb, y_norm, emb_grad, w_rows[0]

    act_spec = P("dp", "tp", None)
    return jax.shard_map(local_step, mesh=mesh, in_specs=(P("dp", None), P("tp", None), P(None), act_spec, act_spec), out_specs=(act_spec, act_spec, P(("tp", "dp"), None), P(None)), check_vma=False)
```

```python
import functools
import math
import jax
import jax.numpy as jnp
import numpy as np
from jax import lax
from jax.sharding import PartitionSpec as P
from jax.experimental import pallas as pl
from jax.experimental.pallas import tpu as pltpu

NORM_EPS = 1e-6
MESH = pl.DeviceIdType.MESH
NDEV = 16
OWN_ROWS = 4096
CAPS = (1536, 576, 368, 368) + (288,) * 4 + (224,) * 8
HALF = tuple(c // 2 for c in CAPS)
HBASE = tuple(sum(HALF[:i]) for i in range(NDEV))
HTOT = sum(HALF)
CAPMAX = max(CAPS)
FAR_CAP = 640
FWD_CHUNKS = 2
ROW_TILE = 64
ACCS = 4
UNROLL = 4
TILE = 128


def coords():
    dp, tp = lax.axis_index("dp"), lax.axis_index("tp")
    return dp // 2, dp % 2, tp // 2, tp % 2


def peer(z, y, x, c, k):
    pz, py, px = (z + k // 4) % 2, (y + (k // 2) % 2) % 2, (x + k % 2) % 2
    dp, tp = pz * 2 + py, px * 2 + c
    return dp, tp, dp * 2 + px


def columns_kernel(g_ref, out_ref, stage, send, recv, fsend, frecv, lsem):
    z, y, x, c = coords()
    dp = z * 2 + y
    q = dp * 2 + x
    cols = out_ref.shape[2]
    partner = (dp, x * 2 + (1 - c))
    barrier = pltpu.get_barrier_semaphore()
    for k in range(1, 8):
        pdp, ptp, _ = peer(z, y, x, c, k)
        pl.semaphore_signal(barrier, inc=1, device_id=(pdp, ptp), device_id_type=MESH)
    pl.semaphore_signal(barrier, inc=1, device_id=partner, device_id_type=MESH)
    pl.semaphore_wait(barrier, 8)

    def block(qq):
        return g_ref.at[:, pl.ds(pl.multiple_of(qq * cols, 128), cols)]

    sends = []
    for k in (7, 3, 5, 6, 1, 2, 4):
        pdp, ptp, pq = peer(z, y, x, c, k)
        cp = pltpu.make_async_remote_copy(
            src_ref=block(pq), dst_ref=out_ref.at[q * 2 + c],
            send_sem=send.at[k], recv_sem=recv.at[k],
            device_id=(pdp, ptp), device_id_type=MESH)
        cp.start()
        sends.append((k, pq, cp))
    fwd = pltpu.make_async_remote_copy(
        src_ref=block(q), dst_ref=out_ref.at[q * 2 + c],
        send_sem=fsend.at[0], recv_sem=frecv.at[0],
        device_id=partner, device_id_type=MESH)
    fwd.start()
    forwards = [fwd]
    cin = pltpu.make_async_copy(block(q), stage, lsem.at[0])
    cin.start()
    cin.wait()
    cout = pltpu.make_async_copy(stage, out_ref.at[q * 2 + c], lsem.at[1])
    cout.start()
    for k, pq, cp in sorted(sends, key=lambda s: bin(s[0]).count("1")):
        cp.wait_recv()
        f = pltpu.make_async_remote_copy(
            src_ref=out_ref.at[pq * 2 + c], dst_ref=out_ref.at[pq * 2 + c],
            send_sem=fsend.at[k], recv_sem=frecv.at[k],
            device_id=partner, device_id_type=MESH)
        f.start()
        forwards.append(f)
    cout.wait()
    for k, pq, cp in sends:
        cp.wait_send()
    for f in forwards:
        f.wait()


def exchange_columns(g):
    rows, width = g.shape
    cols = width // 8
    return pl.pallas_call(
        columns_kernel,
        out_shape=jax.ShapeDtypeStruct((NDEV, rows, cols), g.dtype),
        in_specs=[pl.BlockSpec(memory_space=pl.ANY)],
        out_specs=pl.BlockSpec(memory_space=pl.ANY),
        scratch_shapes=[
            pltpu.VMEM((rows, cols), g.dtype),
            pltpu.SemaphoreType.DMA((8,)),
            pltpu.SemaphoreType.DMA((8,)),
            pltpu.SemaphoreType.DMA((8,)),
            pltpu.SemaphoreType.DMA((8,)),
            pltpu.SemaphoreType.DMA((2,)),
        ],
        compiler_params=pltpu.CompilerParams(collective_id=1, has_side_effects=True),
        name="exchange_columns",
    )(g)


def sum_kernel(rows, tok_rows, work_ref, count_ref, got_ref, acc_ref, *more):
    accs = (acc_ref,) + more
    lanes = len(accs)
    for ref in accs:
        ref[...] = jnp.zeros_like(ref)
    wsum = got_ref[pl.ds(tok_rows, 8), :]
    for s in range(1, NDEV):
        wsum = wsum + got_ref[pl.ds(s * rows + tok_rows, 8), :]
    n = count_ref[0]

    def group(base, refs):
        ws = [work_ref[base + u] for u in range(len(refs))]
        new = [got_ref[pl.ds(w >> 12, 1), :] for w in ws]
        old = [ref[pl.ds(w & 4095, 1), :] for ref, w in zip(refs, ws)]
        for ref, w, a, b in zip(refs, ws, old, new):
            ref[pl.ds(w & 4095, 1), :] = a + b

    def body(i, carry):
        for u in range(UNROLL):
            group((i * UNROLL + u) * lanes, accs)
        return carry

    step = UNROLL * lanes
    lax.fori_loop(0, n // step, body, 0)

    def tail(i, carry):
        group(i, accs[:1])
        return carry

    lax.fori_loop((n // step) * step, n, tail, 0)
    total = accs[0][...]
    for ref in more:
        total = total + ref[...]
    acc_ref[...] = total
    acc_ref[pl.ds(HTOT, 8), :] = wsum


def sum_duplicates(work, count, got, tok_rows):
    _, rows, cols = got.shape
    out_rows = HTOT + 8
    return pl.pallas_call(
        functools.partial(sum_kernel, rows, tok_rows),
        grid_spec=pltpu.PrefetchScalarGridSpec(
            num_scalar_prefetch=2, grid=(1,),
            in_specs=[pl.BlockSpec((NDEV * rows, cols), lambda i, *_: (0, 0))],
            out_specs=pl.BlockSpec((out_rows, cols), lambda i, *_: (0, 0)),
            scratch_shapes=[pltpu.VMEM((out_rows, cols), jnp.float32)] * (ACCS - 1),
        ),
        out_shape=jax.ShapeDtypeStruct((out_rows, cols), jnp.float32),
        compiler_params=pltpu.CompilerParams(vmem_limit_bytes=60 * 2**20),
        name="sum_duplicates",
    )(work, count, got.reshape(NDEV * rows, cols))


def owners_kernel(acc_ref, got_ref, w_ref, send, recv, wsend, wrecv, lsem):
    z, y, x, c = coords()
    dp, tp = z * 2 + y, x * 2 + c
    q = dp * 2 + x
    me = q * 2 + c
    own = tp * 4 + dp
    cols = acc_ref.shape[1]
    lanes = pl.ds(pl.multiple_of(q * cols, 128), cols)
    barrier = pltpu.get_barrier_semaphore()
    for d in range(NDEV):
        @pl.when(own != d)
        def _():
            pl.semaphore_signal(barrier, inc=1, device_id=(d % 4, d // 4), device_id_type=MESH)
    pl.semaphore_wait(barrier, NDEV - 1)

    def remote(d):
        h = HALF[d]
        return pltpu.make_async_remote_copy(
            src_ref=acc_ref.at[pl.ds(HBASE[d], h), :],
            dst_ref=got_ref.at[pl.ds(pl.multiple_of(c * h, 8), h), lanes],
            send_sem=send.at[d], recv_sem=recv.at[me],
            device_id=(d % 4, d // 4), device_id_type=MESH)

    def local(d):
        h = HALF[d]
        return pltpu.make_async_copy(
            acc_ref.at[pl.ds(HBASE[d], h), :],
            got_ref.at[pl.ds(pl.multiple_of(c * h, 8), h), lanes], lsem.at[0])

    wrow = acc_ref.at[pl.ds(HTOT, 8), :]

    def wcopy(k):
        pdp, ptp, _ = peer(z, y, x, c, k)
        return pltpu.make_async_remote_copy(
            src_ref=wrow, dst_ref=w_ref.at[:, lanes],
            send_sem=wsend.at[k], recv_sem=wrecv.at[k],
            device_id=(pdp, ptp), device_id_type=MESH)

    for k in range(1, 8):
        wcopy(k).start()
    wlocal = pltpu.make_async_copy(wrow, w_ref.at[:, lanes], lsem.at[1])
    wlocal.start()
    for d in range(NDEV):
        @pl.when(own != d)
        def _():
            remote(d).start()

        @pl.when(own == d)
        def _():
            local(d).start()
    for k in range(1, 8):
        wcopy(k).wait()
    wlocal.wait()
    for d in range(NDEV):
        h = HALF[d]

        @pl.when(own == d)
        def _():
            local(d).wait()
            for s in range(NDEV):
                @pl.when(me != s)
                def _():
                    pltpu.make_async_remote_copy(
                        src_ref=acc_ref.at[pl.ds(HBASE[d], h), :],
                        dst_ref=got_ref.at[pl.ds((s % 2) * h, h), pl.ds((s // 2) * cols, cols)],
                        send_sem=send.at[d], recv_sem=recv.at[s],
                        device_id=(s // 4, s % 4), device_id_type=MESH).wait_recv()

        @pl.when(own != d)
        def _():
            remote(d).wait_send()


def send_to_owners(acc):
    cols = acc.shape[1]
    return pl.pallas_call(
        owners_kernel,
        out_shape=(jax.ShapeDtypeStruct((CAPMAX, cols * 8), jnp.float32),
                   jax.ShapeDtypeStruct((8, cols * 8), jnp.float32)),
        in_specs=[pl.BlockSpec(memory_space=pltpu.VMEM)],
        out_specs=(pl.BlockSpec(memory_space=pl.ANY), pl.BlockSpec(memory_space=pl.ANY)),
        scratch_shapes=[
            pltpu.SemaphoreType.DMA((NDEV,)),
            pltpu.SemaphoreType.DMA((NDEV,)),
            pltpu.SemaphoreType.DMA((8,)),
            pltpu.SemaphoreType.DMA((8,)),
            pltpu.SemaphoreType.DMA((2,)),
        ],
        compiler_params=pltpu.CompilerParams(collective_id=2, has_side_effects=True),
        name="send_to_owners",
    )(acc)


def expand_kernel(scale, bounds_ref, ids_ref, got_ref, out_ref):
    t = pl.program_id(0)
    half = bounds_ref[OWN_ROWS // TILE + 1]
    base = bounds_ref[OWN_ROWS // TILE + 2] + t * TILE
    out_ref[...] = jnp.zeros_like(out_ref)

    lo, hi = bounds_ref[t], bounds_ref[t + 1]

    def copy(slots):
        rows = [got_ref[pl.ds((s & 1) * half + (s >> 1), 1), :] * scale for s in slots]
        for s, row in zip(slots, rows):
            out_ref[pl.ds(ids_ref[s] - base, 1), :] = row

    def body(i, carry):
        copy([lo + i * 2, lo + i * 2 + 1])
        return carry

    pairs = (hi - lo) // 2
    lax.fori_loop(0, pairs, body, 0)

    @pl.when((hi - lo) % 2 == 1)
    def _():
        copy([hi - 1])


def expand(bounds, ids, got, scale):
    width = got.shape[1]
    return pl.pallas_call(
        functools.partial(expand_kernel, scale),
        grid_spec=pltpu.PrefetchScalarGridSpec(
            num_scalar_prefetch=2, grid=(OWN_ROWS // TILE,),
            in_specs=[pl.BlockSpec((CAPMAX, width), lambda i, *_: (0, 0))],
            out_specs=pl.BlockSpec((TILE, width), lambda i, *_: (i, 0)),
        ),
        out_shape=jax.ShapeDtypeStruct((OWN_ROWS, width), jnp.float32),
        compiler_params=pltpu.CompilerParams(vmem_limit_bytes=60 * 2**20),
        name="expand",
    )(bounds, ids, got)


def norm_kernel(c_ref, slots_ref, near_ref, mine0, mine1, theirs0, theirs1, dyn_ref, dyr_ref, w_ref,
                x_ref, y_ref, g_ref, far, picked, wacc, sems):
    t = pl.program_id(0)
    last = pl.num_programs(0) - 1
    half = FAR_CAP // 2
    width = w_ref.shape[1]

    @pl.when(t == 0)
    def _():
        wacc[...] = jnp.zeros_like(wacc)
        copies = []
        for j, (ref, core) in enumerate(((mine0, c_ref[0]), (mine1, c_ref[0]), (theirs0, 1 - c_ref[0]), (theirs1, 1 - c_ref[0]))):
            at = pl.multiple_of(core * half + (j % 2) * (half // 2), 8)
            copies.append(pltpu.make_async_copy(ref, far.at[pl.ds(at, half // 2), :], sems.at[j]))
        for cp in copies:
            cp.start()
        far[pl.ds(FAR_CAP, 8), :] = jnp.zeros((8, width), jnp.float32)
        for cp in copies:
            cp.wait()

    @pl.when(t < last)
    def _():
        def pick(i, carry):
            rows = [far[pl.ds(slots_ref[t * ROW_TILE + i * 4 + u], 1), :] for u in range(4)]
            for u in range(4):
                picked[pl.ds(i * 4 + u, 1), :] = rows[u]
            return carry

        lax.fori_loop(0, ROW_TILE // 4, pick, 0)
        gain = 1.0 + w_ref[...]

        def body(i, carry):
            at = pl.ds(pl.multiple_of(i * 16, 16), 16)
            xb = (near_ref[at, :] + picked[at, :]).astype(jnp.bfloat16)
            x_ref[at, :] = xb
            xf = xb.astype(jnp.float32)
            r = lax.rsqrt(jnp.sum(xf * xf, axis=1, keepdims=True) * (1.0 / width) + NORM_EPS)
            xh = xf * r
            y_ref[at, :] = (xh * gain).astype(jnp.bfloat16)
            dy = dyn_ref[at, :].astype(jnp.float32)
            wacc[...] += dy * xh
            a = dy * gain
            m = jnp.sum(a * xh, axis=1, keepdims=True) * (1.0 / width)
            g_ref[at, :] = dyr_ref[at, :].astype(jnp.float32) + r * (a - xh * m)
            return carry

        lax.fori_loop(0, ROW_TILE // 16, body, 0)

    @pl.when(t == last)
    def _():
        total = jnp.sum(wacc[...], axis=0, keepdims=True)
        first = lax.broadcasted_iota(jnp.int32, (8, width), 0) == 0
        g_ref[pl.ds(0, 8), :] = jnp.where(first, total, 0.0)


def norm(core, slots, near, far, dyn, dyr, w):
    rows, width = near.shape
    tiles = rows // ROW_TILE
    row = pl.BlockSpec((ROW_TILE, width), lambda i, *_: (jnp.minimum(i, tiles - 1), 0))
    anyspec = pl.BlockSpec(memory_space=pl.ANY)
    return pl.pallas_call(
        norm_kernel,
        grid_spec=pltpu.PrefetchScalarGridSpec(
            num_scalar_prefetch=2, grid=(tiles + 1,),
            in_specs=[row] + [anyspec] * 4 + [row, row, pl.BlockSpec((1, width), lambda i, *_: (0, 0))],
            out_specs=[row, row, pl.BlockSpec((ROW_TILE, width), lambda i, *_: (i, 0))],
            scratch_shapes=[
                pltpu.VMEM((FAR_CAP + 8, width), jnp.float32),
                pltpu.VMEM((ROW_TILE, width), jnp.float32),
                pltpu.VMEM((16, width), jnp.float32),
                pltpu.SemaphoreType.DMA((4,)),
            ],
        ),
        out_shape=(jax.ShapeDtypeStruct((rows, width), jnp.bfloat16),
                   jax.ShapeDtypeStruct((rows, width), jnp.bfloat16),
                   jax.ShapeDtypeStruct((rows + 8, width), jnp.float32)),
        compiler_params=pltpu.CompilerParams(vmem_limit_bytes=60 * 2**20),
        name="assemble_norm",
    )(core, slots, near, *far, dyn, dyr, w)


def solution(mesh):
    def plan(all_ids, rows):
        n = all_ids.shape[0]
        dp, tp = lax.axis_index("dp"), lax.axis_index("tp")
        me, core = tp * 4 + dp, tp % 2
        keys = lax.sort(all_ids * n + lax.iota(jnp.int32, n), is_stable=False)
        ids, idx = keys >> 13, keys & (n - 1)
        differs = ids[1:] != ids[:-1]
        one = jnp.ones((1,), jnp.int32)
        first = jnp.concatenate([one, differs.astype(jnp.int32)])
        slot = jnp.cumsum(first) - 1
        edges = jnp.arange(NDEV + 1, dtype=jnp.int32) * OWN_ROWS
        starts = jnp.sum(jnp.where(ids[None, :] < edges[:, None], first[None, :], 0), axis=1)
        caps = jnp.array(CAPS, jnp.int32)
        overflow = jnp.any(starts[1:] - starts[:-1] > caps)
        chip = idx >> 10
        fresh = jnp.concatenate([one, (differs | (chip[1:] != chip[:-1])).astype(jnp.int32)])
        far = jnp.where((ids >> 15) != (chip & 1), fresh, 0)
        per_chip = jnp.sum(jnp.where(chip[None, :] == jnp.arange(8, dtype=jnp.int32)[:, None], far[None, :], 0), axis=1)
        overflow = overflow | jnp.any(per_chip > FAR_CAP)
        owner = ids // OWN_ROWS
        hit = owner[None, :] == jnp.arange(NDEV, dtype=jnp.int32)[:, None]
        offset = jnp.sum(jnp.where(hit, starts[:-1][:, None], 0), axis=0)
        hbase = jnp.sum(jnp.where(hit, jnp.array(HBASE, jnp.int32)[:, None], 0), axis=0)
        local_slot = slot - offset
        pos = jnp.minimum(hbase + local_slot // 2, HTOT - 1)
        mine = local_slot % 2 == core
        src = (idx // 512) * rows + idx % 512
        work = lax.sort(jnp.where(mine, 0, 1 << 26) + src * 4096 + pos, is_stable=False)
        count = jnp.sum(mine.astype(jnp.int32)).reshape(1)
        uniq = lax.sort(jnp.where(first == 1, ids, 1 << 20), is_stable=False)
        uniq = jnp.concatenate([uniq, jnp.full((CAPMAX,), 1 << 20, jnp.int32)])
        my_start = jnp.sum(jnp.where(jnp.arange(NDEV) == me, starts[:-1], 0))
        my_ids = lax.dynamic_slice(uniq, (my_start,), (CAPMAX,))
        tiles = me * OWN_ROWS + jnp.arange(OWN_ROWS // TILE + 1, dtype=jnp.int32) * TILE
        bounds = jnp.sum(jnp.where(ids[None, :] < tiles[:, None], first[None, :], 0), axis=1) - my_start
        my_half = jnp.sum(jnp.where(jnp.arange(NDEV) == me, jnp.array(HALF, jnp.int32), 0))
        bounds = jnp.concatenate([bounds, my_half[None], (me * OWN_ROWS)[None]]).astype(jnp.int32)
        return overflow, work, count, my_ids, bounds

    def far_lists(ids):
        n = ids.shape[1]
        pos = lax.iota(jnp.int32, n)
        same = ids[:, :, None] == ids[:, None, :]
        lead = jnp.min(jnp.where(same, pos[None, :, None], n), axis=1)
        far = (ids >> 15) != jnp.arange(2, dtype=jnp.int32)[:, None]
        first = (lead == pos[None]) & far
        slot = jnp.sum(jnp.where(first[:, :, None] & (pos[None, :, None] < lead[:, None, :]), 1, 0), axis=1)
        slots = lax.iota(jnp.int32, FAR_CAP)
        at = first[:, :, None] & (slot[:, :, None] == slots[None, None, :])
        listed = jnp.max(jnp.where(at, ids[:, :, None], -1), axis=1)
        return listed, jnp.where(far, jnp.minimum(slot, FAR_CAP - 1), FAR_CAP)

    def local_step(tokens, emb_table, w_norm, dy_norm, dy_resid):
        shard_rows, model_dim = emb_table.shape
        scale_float = jnp.asarray(math.sqrt(model_dim), jnp.bfloat16).astype(jnp.float32)
        scale_py = float(np.array(math.sqrt(model_dim)).astype(jnp.dtype(jnp.bfloat16)))
        dp, tp = lax.axis_index("dp"), lax.axis_index("tp")
        x, c = tp // 2, tp % 2
        seq = tokens.shape[1]
        part = seq // 4
        swap_core = [(t, t ^ 1) for t in range(4)]
        swap_x = [(t, t ^ 2) for t in range(4)]

        def fetch(ids):
            ids = ids - tp * shard_rows
            owned = (ids >= 0) & (ids < shard_rows)
            got = jnp.take(emb_table, jnp.where(owned, ids, 0), axis=0, mode="clip")
            return jnp.where(owned[:, None], got.astype(jnp.float32) * scale_float, 0.0)

        def positions(toks, px, pc):
            return lax.dynamic_slice(toks, ((px * 2 + pc) * part,), (part,))

        listed, slots = far_lists(tokens.reshape(2, seq // 2))
        my_list = jnp.where(x == 0, listed[1], listed[0])
        my_slots = lax.dynamic_slice(slots.reshape(-1), (tp * part,), (part,))
        half, n = FAR_CAP // 2, FAR_CAP // 2 // FWD_CHUNKS
        got, toks = [], tokens[0]
        for k in range(FWD_CHUNKS):
            theirs = lax.dynamic_slice(my_list, ((1 - c) * half + k * n,), (n,))
            mine = lax.dynamic_slice(my_list, (c * half + k * n,), (n,))
            both = fetch(theirs)
            both = lax.ppermute(both, "tp", swap_core)
            both = both + fetch(mine)
            both, my_list, toks = lax.optimization_barrier((both, my_list, toks))
            got.append(lax.ppermute(both, "tp", swap_x))
        relayed = [lax.ppermute(r, "tp", swap_core) for r in got]
        all_ids = lax.all_gather(toks[None], "dp", axis=0, tiled=True).reshape(-1)
        near = fetch(positions(toks, x, 1 - c))
        near = lax.ppermute(near, "tp", swap_core)
        near = near + fetch(positions(toks, x, c))
        rows = part + 8
        overflow, work, count, my_ids, bounds = plan(all_ids, rows)

        def dense_forward(near, toks):
            far = lax.ppermute(fetch(positions(toks, 1 - x, 1 - c)), "tp", swap_core) + fetch(positions(toks, 1 - x, c))
            x_emb = (near + lax.ppermute(far, "tp", swap_x)).astype(jnp.bfloat16)
            x_float = x_emb.astype(jnp.float32)
            inv_rms = lax.rsqrt(jnp.mean(x_float * x_float, axis=-1, keepdims=True) + NORM_EPS)
            x_hat = x_float * inv_rms
            norm_gain = 1.0 + w_norm
            y_norm = (x_hat * norm_gain).astype(jnp.bfloat16)
            dy_float = dy_norm[0].astype(jnp.float32)
            dx_hat = dy_float * norm_gain
            tok_grad = dy_resid[0].astype(jnp.float32) + inv_rms * (dx_hat - x_hat * jnp.mean(dx_hat * x_hat, axis=-1, keepdims=True))
            w_part = jnp.sum(dy_float * x_hat, axis=0)
            return x_emb, y_norm, jnp.concatenate([tok_grad, jnp.pad(w_part[None], ((0, 7), (0, 0)))], axis=0)

        def sparse_forward(near, toks):
            core = c.astype(jnp.int32).reshape(1)
            return tuple(norm(core, my_slots, near, got + relayed, dy_norm[0], dy_resid[0], w_norm[None]))

        x_emb, y_norm, g_ext = lax.cond(overflow, dense_forward, sparse_forward, near, toks)

        cols = exchange_columns(g_ext)
        acc = sum_duplicates(work, count, cols, part)
        owned, w_rows = send_to_owners(acc)

        def dense_backward(g_ext, owned):
            g = g_ext[:part]
            ids = tokens[0] - tp * shard_rows
            seq_grad = jnp.zeros((seq, model_dim), jnp.float32)
            for s in range(4):
                block = g if s == 0 else lax.ppermute(g, "tp", [(t, (t + s) % 4) for t in range(4)])
                seq_grad = lax.dynamic_update_slice(seq_grad, block, ((tp + 4 - s) % 4 * part, 0))
            drop_ids = jnp.where((ids >= 0) & (ids < shard_rows), ids, shard_rows)
            shard_grad = jax.ops.segment_sum(seq_grad, drop_ids, num_segments=shard_rows, mode="drop") * scale_float
            total = lax.dynamic_slice(shard_grad, (dp * OWN_ROWS, 0), (OWN_ROWS, model_dim))
            for s in range(1, 4):
                block = lax.dynamic_slice(shard_grad, ((dp + s) % 4 * OWN_ROWS, 0), (OWN_ROWS, model_dim))
                total = total + lax.ppermute(block, "dp", [(d, (d + s) % 4) for d in range(4)])
            return total

        def sparse_backward(g_ext, owned):
            return expand(bounds, my_ids, owned, scale_py)

        emb_grad = lax.cond(overflow, dense_backward, sparse_backward, g_ext, owned)
        return x_emb[None], y_norm[None], emb_grad, w_rows[0]

    act_spec = P("dp", "tp", None)
    return jax.shard_map(local_step, mesh=mesh, in_specs=(P("dp", None), P("tp", None), P(None), act_spec, act_spec), out_specs=(act_spec, act_spec, P(("tp", "dp"), None), P(None)), check_vma=False)
```

```python
import functools
import math
import jax
import jax.numpy as jnp
import numpy as np
from jax import lax
from jax.sharding import PartitionSpec as P
from jax.experimental import pallas as pl
from jax.experimental.pallas import tpu as pltpu

NORM_EPS = 1e-6
MESH = pl.DeviceIdType.MESH
NDEV = 16
OWN_ROWS = 4096
CAPS = (1536, 544, 352, 352) + (256,) * 4 + (208,) * 8
HALF = tuple(c // 2 for c in CAPS)
HBASE = tuple(sum(HALF[:i]) for i in range(NDEV))
HTOT = sum(HALF)
CAPMAX = max(CAPS)
FAR_CAP = 640
FAR_CHUNKS = (128, 192)
NEAR_PIECE = 256
ROW_TILE = 64
ACCS = 4
UNROLL = 4
TILE = 128


def coords():
    dp, tp = lax.axis_index("dp"), lax.axis_index("tp")
    return dp // 2, dp % 2, tp // 2, tp % 2


def flip(pos, dims):
    z, y, x, c = pos
    return ((1 - z if 2 in dims else z), (1 - y if 1 in dims else y), (1 - x if 0 in dims else x), c)


def chip_of(pos):
    z, y, x, _ = pos
    return z * 4 + y * 2 + x


def device_of(pos):
    z, y, x, c = pos
    return z * 2 + y, x * 2 + c


def bits(k):
    return tuple(d for d in range(3) if k >> d & 1)


def hops(third, k):
    return tuple(d for d in ((third + i) % 3 for i in range(3)) if k >> d & 1)


def kinds(third):
    a, b, c = (1 << ((third + i) % 3) for i in range(3))
    return (7, a + b, a + c, b + c, a, b, c)


HOP_ID = {}
for _t in range(3):
    for _k in range(1, 8):
        for _h in range(len(hops(_t, _k))):
            HOP_ID[_t, _k, _h] = len(HOP_ID)
RELAY_ID = {}
for _t, _k, _h in HOP_ID:
    if _h + 1 < len(hops(_t, _k)):
        RELAY_ID[_t, _k, _h] = len(RELAY_ID)


def columns_kernel(g_ref, out_ref, stage, relay, send, recv, fsend, frecv, lsem):
    me = coords()
    q, c = chip_of(me), me[3]
    cols = out_ref.shape[2]
    third = cols // 3
    partner = device_of(me[:3] + (1 - c,))
    barrier = pltpu.get_barrier_semaphore()
    for d in range(3):
        pl.semaphore_signal(barrier, inc=1, device_id=device_of(flip(me, (d,))), device_id_type=MESH)
    pl.semaphore_signal(barrier, inc=1, device_id=partner, device_id_type=MESH)
    pl.semaphore_wait(barrier, 4)

    def block(chip, at, width):
        return g_ref.at[:, pl.ds(pl.multiple_of(chip * cols + at, 128), width)]

    def landed(src, t):
        return out_ref.at[chip_of(src) * 2 + c, :, pl.ds(t * third, third)]

    def hop(t, k, h):
        dims = hops(t, k)
        if h == 0:
            src = block(chip_of(flip(me, dims)), t * third, third)
        else:
            src = relay.at[RELAY_ID[t, k, h - 1]]
        if h + 1 < len(dims):
            dst = relay.at[RELAY_ID[t, k, h]]
        else:
            dst = landed(flip(me, dims[:h]), t)
        n = HOP_ID[t, k, h]
        return pltpu.make_async_remote_copy(
            src_ref=src, dst_ref=dst, send_sem=send.at[n], recv_sem=recv.at[n],
            device_id=device_of(flip(me, dims[h:h + 1])), device_id_type=MESH)

    for i in range(7):
        for t in range(3):
            hop(t, kinds(t)[i], 0).start()
    own = pltpu.make_async_remote_copy(
        src_ref=block(q, 0, cols), dst_ref=out_ref.at[q * 2 + c],
        send_sem=fsend.at[0], recv_sem=frecv.at[0],
        device_id=partner, device_id_type=MESH)
    own.start()
    cin = pltpu.make_async_copy(block(q, 0, cols), stage, lsem.at[0])
    cin.start()
    cin.wait()
    cout = pltpu.make_async_copy(stage, out_ref.at[q * 2 + c], lsem.at[1])
    cout.start()
    for i, h in ((0, 1), (1, 1), (2, 1), (3, 1), (0, 2)):
        for t in range(3):
            k = kinds(t)[i]
            hop(t, k, h - 1).wait_recv()
            hop(t, k, h).start()
    forwards = []
    for i in (4, 5, 6, 1, 2, 3, 0):
        for t in range(3):
            k = kinds(t)[i]
            hop(t, k, len(hops(t, k)) - 1).wait_recv()
            here = landed(flip(me, bits(k)), t)
            f = pltpu.make_async_remote_copy(
                src_ref=here, dst_ref=here,
                send_sem=fsend.at[k * 3 + t], recv_sem=frecv.at[k * 3 + t],
                device_id=partner, device_id_type=MESH)
            f.start()
            forwards.append(f)
    cout.wait()
    for t, k, h in HOP_ID:
        hop(t, k, h).wait_send()
    own.wait()
    for f in forwards:
        f.wait()


def exchange_columns(g):
    rows, width = g.shape
    cols = width // 8
    return pl.pallas_call(
        columns_kernel,
        out_shape=jax.ShapeDtypeStruct((NDEV, rows, cols), g.dtype),
        in_specs=[pl.BlockSpec(memory_space=pl.ANY)],
        out_specs=pl.BlockSpec(memory_space=pl.ANY),
        scratch_shapes=[
            pltpu.VMEM((rows, cols), g.dtype),
            pltpu.VMEM((len(RELAY_ID), rows, cols // 3), g.dtype),
            pltpu.SemaphoreType.DMA((len(HOP_ID),)),
            pltpu.SemaphoreType.DMA((len(HOP_ID),)),
            pltpu.SemaphoreType.DMA((24,)),
            pltpu.SemaphoreType.DMA((24,)),
            pltpu.SemaphoreType.DMA((2,)),
        ],
        compiler_params=pltpu.CompilerParams(collective_id=1, has_side_effects=True),
        name="exchange_columns",
    )(g)


def sum_kernel(rows, tok_rows, work_ref, count_ref, got_ref, acc_ref, *more):
    accs = (acc_ref,) + more
    lanes = len(accs)
    for ref in accs:
        ref[...] = jnp.zeros_like(ref)
    wsum = got_ref[pl.ds(tok_rows, 8), :]
    for s in range(1, NDEV):
        wsum = wsum + got_ref[pl.ds(s * rows + tok_rows, 8), :]
    n = count_ref[0]

    def group(base, refs):
        ws = [work_ref[base + u] for u in range(len(refs))]
        new = [got_ref[pl.ds(w >> 12, 1), :] for w in ws]
        old = [ref[pl.ds(w & 4095, 1), :] for ref, w in zip(refs, ws)]
        for ref, w, a, b in zip(refs, ws, old, new):
            ref[pl.ds(w & 4095, 1), :] = a + b

    def body(i, carry):
        for u in range(UNROLL):
            group((i * UNROLL + u) * lanes, accs)
        return carry

    step = UNROLL * lanes
    lax.fori_loop(0, n // step, body, 0)

    def tail(i, carry):
        group(i, accs[:1])
        return carry

    lax.fori_loop((n // step) * step, n, tail, 0)
    total = accs[0][...]
    for ref in more:
        total = total + ref[...]
    acc_ref[...] = total
    acc_ref[pl.ds(HTOT, 8), :] = wsum


def sum_duplicates(work, count, got, tok_rows):
    _, rows, cols = got.shape
    out_rows = HTOT + 8
    return pl.pallas_call(
        functools.partial(sum_kernel, rows, tok_rows),
        grid_spec=pltpu.PrefetchScalarGridSpec(
            num_scalar_prefetch=2, grid=(1,),
            in_specs=[pl.BlockSpec((NDEV * rows, cols), lambda i, *_: (0, 0))],
            out_specs=pl.BlockSpec((out_rows, cols), lambda i, *_: (0, 0)),
            scratch_shapes=[pltpu.VMEM((out_rows, cols), jnp.float32)] * (ACCS - 1),
        ),
        out_shape=jax.ShapeDtypeStruct((out_rows, cols), jnp.float32),
        compiler_params=pltpu.CompilerParams(vmem_limit_bytes=60 * 2**20),
        name="sum_duplicates",
    )(work, count, got.reshape(NDEV * rows, cols))


RELAYS = {3: 2, 5: 1, 6: 4}
RELAYED = {r: q for q, r in RELAYS.items()}
NEIGHBOURS = (1, 2, 4)


def owners_kernel(acc_ref, got_ref, w_ref, relay, send, recv, wsend, wrecv, psend, precv, rsend, rrecv, lsem):
    me = coords()
    q, c = chip_of(me), me[3]
    dp, tp = device_of(me)
    src = q * 2 + c
    own = tp * 4 + dp
    cols = acc_ref.shape[1]
    third = cols // 3
    big = HALF[0]
    lanes = pl.ds(pl.multiple_of(q * cols, 128), cols)
    barrier = pltpu.get_barrier_semaphore()
    for d in range(NDEV):
        @pl.when(own != d)
        def _():
            pl.semaphore_signal(barrier, inc=1, device_id=(d % 4, d // 4), device_id_type=MESH)
    pl.semaphore_wait(barrier, NDEV - 1)

    def rows_on(d, core):
        return pl.ds(pl.multiple_of(core * HALF[d], 8), HALF[d])

    def remote(d):
        return pltpu.make_async_remote_copy(
            src_ref=acc_ref.at[pl.ds(HBASE[d], HALF[d]), :], dst_ref=got_ref.at[rows_on(d, c), lanes],
            send_sem=send.at[d], recv_sem=recv.at[src],
            device_id=(d % 4, d // 4), device_id_type=MESH)

    def local(d):
        return pltpu.make_async_copy(
            acc_ref.at[pl.ds(HBASE[d], HALF[d]), :], got_ref.at[rows_on(d, c), lanes], lsem.at[0])

    def to_relay(chip, t, slot):
        return pltpu.make_async_remote_copy(
            src_ref=acc_ref.at[pl.ds(HBASE[0], big), pl.ds(t * third, third)], dst_ref=relay.at[slot],
            send_sem=rsend.at[t], recv_sem=rrecv.at[slot],
            device_id=(chip // 2, (chip % 2) * 2 + c), device_id_type=MESH)

    def passed(slot, from_chip, t):
        return pltpu.make_async_remote_copy(
            src_ref=relay.at[slot],
            dst_ref=got_ref.at[rows_on(0, c), pl.ds(from_chip * cols + t * third, third)],
            send_sem=psend.at[slot], recv_sem=precv.at[(from_chip * 2 + c) * 3 + t],
            device_id=(0, 0), device_id_type=MESH)

    wrow = acc_ref.at[pl.ds(HTOT, 8), :]

    def wcopy(k):
        return pltpu.make_async_remote_copy(
            src_ref=wrow, dst_ref=w_ref.at[:, lanes],
            send_sem=wsend.at[k], recv_sem=wrecv.at[k],
            device_id=device_of(flip(me, bits(k))), device_id_type=MESH)

    direct0 = (q == 1) | (q == 2) | (q == 4) | (src == 1)
    for chip, via in RELAYS.items():
        @pl.when(q == chip)
        def _():
            for t in range(3):
                to_relay(via, t, t).start()

    @pl.when(q == 7)
    def _():
        for t in range(3):
            to_relay(NEIGHBOURS[t], t, 3).start()

    @pl.when(direct0)
    def _():
        remote(0).start()

    @pl.when(own == 0)
    def _():
        local(0).start()

    for d in range(1, NDEV):
        @pl.when(own != d)
        def _():
            remote(d).start()

        @pl.when(own == d)
        def _():
            local(d).start()
    for k in range(1, 8):
        wcopy(k).start()
    wlocal = pltpu.make_async_copy(wrow, w_ref.at[:, lanes], lsem.at[1])
    wlocal.start()

    for i, chip in enumerate(NEIGHBOURS):
        @pl.when(q == chip)
        def _():
            for slot in range(4):
                to_relay(chip, 0, slot).wait_recv()
                passed(slot, 7 if slot == 3 else RELAYED[chip], i if slot == 3 else slot).start()

    for k in range(1, 8):
        wcopy(k).wait()
    wlocal.wait()

    def arrived(d, s):
        h = HALF[d]
        return pltpu.make_async_remote_copy(
            src_ref=acc_ref.at[pl.ds(HBASE[d], h), :],
            dst_ref=got_ref.at[pl.ds((s % 2) * h, h), pl.ds((s // 2) * cols, cols)],
            send_sem=send.at[d], recv_sem=recv.at[s],
            device_id=(0, 0), device_id_type=MESH)

    def arrived_third(s, t):
        return pltpu.make_async_remote_copy(
            src_ref=relay.at[0],
            dst_ref=got_ref.at[pl.ds((s % 2) * big, big), pl.ds((s // 2) * cols + t * third, third)],
            send_sem=psend.at[0], recv_sem=precv.at[s * 3 + t],
            device_id=(0, 0), device_id_type=MESH)

    for d in range(NDEV):
        @pl.when(own == d)
        def _():
            local(d).wait()
            for s in range(NDEV):
                if d == 0 and s // 2 in (3, 5, 6, 7):
                    for t in range(3):
                        arrived_third(s, t).wait_recv()
                elif d == 0:
                    if s > 0:
                        arrived(d, s).wait_recv()
                else:
                    @pl.when(src != s)
                    def _():
                        arrived(d, s).wait_recv()

        if d > 0:
            @pl.when(own != d)
            def _():
                remote(d).wait_send()

    @pl.when(direct0)
    def _():
        remote(0).wait_send()

    for chip, via in RELAYS.items():
        @pl.when(q == chip)
        def _():
            for t in range(3):
                to_relay(via, t, t).wait_send()

    @pl.when(q == 7)
    def _():
        for t in range(3):
            to_relay(NEIGHBOURS[t], t, 3).wait_send()

    for i, chip in enumerate(NEIGHBOURS):
        @pl.when(q == chip)
        def _():
            for slot in range(4):
                passed(slot, 7 if slot == 3 else RELAYED[chip], i if slot == 3 else slot).wait_send()


def send_to_owners(acc):
    cols = acc.shape[1]
    return pl.pallas_call(
        owners_kernel,
        out_shape=(jax.ShapeDtypeStruct((CAPMAX, cols * 8), jnp.float32),
                   jax.ShapeDtypeStruct((8, cols * 8), jnp.float32)),
        in_specs=[pl.BlockSpec(memory_space=pltpu.VMEM)],
        out_specs=(pl.BlockSpec(memory_space=pl.ANY), pl.BlockSpec(memory_space=pl.ANY)),
        scratch_shapes=[
            pltpu.VMEM((4, HALF[0], cols // 3), jnp.float32),
            pltpu.SemaphoreType.DMA((NDEV,)),
            pltpu.SemaphoreType.DMA((NDEV,)),
            pltpu.SemaphoreType.DMA((8,)),
            pltpu.SemaphoreType.DMA((8,)),
            pltpu.SemaphoreType.DMA((4,)),
            pltpu.SemaphoreType.DMA((NDEV * 3,)),
            pltpu.SemaphoreType.DMA((3,)),
            pltpu.SemaphoreType.DMA((4,)),
            pltpu.SemaphoreType.DMA((2,)),
        ],
        compiler_params=pltpu.CompilerParams(collective_id=2, has_side_effects=True),
        name="send_to_owners",
    )(acc)


def expand_kernel(scale, bounds_ref, ids_ref, got_ref, out_ref):
    t = pl.program_id(0)
    half = bounds_ref[OWN_ROWS // TILE + 1]
    base = bounds_ref[OWN_ROWS // TILE + 2] + t * TILE
    out_ref[...] = jnp.zeros_like(out_ref)

    lo, hi = bounds_ref[t], bounds_ref[t + 1]

    def copy(slots):
        rows = [got_ref[pl.ds((s & 1) * half + (s >> 1), 1), :] * scale for s in slots]
        for s, row in zip(slots, rows):
            out_ref[pl.ds(ids_ref[s] - base, 1), :] = row

    def body(i, carry):
        copy([lo + i * 2, lo + i * 2 + 1])
        return carry

    pairs = (hi - lo) // 2
    lax.fori_loop(0, pairs, body, 0)

    @pl.when((hi - lo) % 2 == 1)
    def _():
        copy([hi - 1])


def expand(bounds, ids, got, scale):
    width = got.shape[1]
    return pl.pallas_call(
        functools.partial(expand_kernel, scale),
        grid_spec=pltpu.PrefetchScalarGridSpec(
            num_scalar_prefetch=2, grid=(OWN_ROWS // TILE,),
            in_specs=[pl.BlockSpec((CAPMAX, width), lambda i, *_: (0, 0))],
            out_specs=pl.BlockSpec((TILE, width), lambda i, *_: (i, 0)),
        ),
        out_shape=jax.ShapeDtypeStruct((OWN_ROWS, width), jnp.float32),
        compiler_params=pltpu.CompilerParams(vmem_limit_bytes=60 * 2**20),
        name="expand",
    )(bounds, ids, got)


def norm_kernel(c_ref, slots_ref, own0, own1, theirs0, theirs1, mine_a, mine_b, his_a, his_b,
                dyn_ref, dyr_ref, w_ref, x_ref, y_ref, g_ref, far, picked, wacc, sems):
    t = pl.program_id(0)
    last = pl.num_programs(0) - 1
    half = FAR_CAP // 2
    width = w_ref.shape[1]

    @pl.when(t == 0)
    def _():
        wacc[...] = jnp.zeros_like(wacc)
        copies = []
        for j, ref in enumerate((mine_a, mine_b, his_a, his_b)):
            core = c_ref[0] if j < 2 else 1 - c_ref[0]
            at = pl.multiple_of(core * half + (j % 2) * FAR_CHUNKS[0], 8)
            copies.append(pltpu.make_async_copy(ref, far.at[pl.ds(at, FAR_CHUNKS[j % 2]), :], sems.at[j]))
        for cp in copies:
            cp.start()
        far[pl.ds(FAR_CAP, 8), :] = jnp.zeros((8, width), jnp.float32)
        for cp in copies:
            cp.wait()

    @pl.when(t < last)
    def _():
        def pick(i, carry):
            rows = [far[pl.ds(slots_ref[t * ROW_TILE + i * 8 + u], 1), :] for u in range(8)]
            for u in range(8):
                picked[pl.ds(i * 8 + u, 1), :] = rows[u]
            return carry

        lax.fori_loop(0, ROW_TILE // 8, pick, 0)
        gain = 1.0 + w_ref[...]

        def piece(own, theirs):
            def body(i, carry):
                at = pl.ds(pl.multiple_of(i * 16, 16), 16)
                xb = (own[at, :] + theirs[at, :] + picked[at, :]).astype(jnp.bfloat16)
                x_ref[at, :] = xb
                xf = xb.astype(jnp.float32)
                r = lax.rsqrt(jnp.sum(xf * xf, axis=1, keepdims=True) * (1.0 / width) + NORM_EPS)
                xh = xf * r
                y_ref[at, :] = (xh * gain).astype(jnp.bfloat16)
                dy = dyn_ref[at, :].astype(jnp.float32)
                wacc[...] += dy * xh
                a = dy * gain
                m = jnp.sum(a * xh, axis=1, keepdims=True) * (1.0 / width)
                g_ref[at, :] = dyr_ref[at, :].astype(jnp.float32) + r * (a - xh * m)
                return carry

            lax.fori_loop(0, ROW_TILE // 16, body, 0)

        @pl.when(t < NEAR_PIECE // ROW_TILE)
        def _():
            piece(own0, theirs0)

        @pl.when(t >= NEAR_PIECE // ROW_TILE)
        def _():
            piece(own1, theirs1)

    @pl.when(t == last)
    def _():
        total = jnp.sum(wacc[...], axis=0, keepdims=True)
        first = lax.broadcasted_iota(jnp.int32, (8, width), 0) == 0
        g_ref[pl.ds(0, 8), :] = jnp.where(first, total, 0.0)


def norm(core, slots, own, theirs, far, dyn, dyr, w):
    rows, width = dyn.shape
    tiles = rows // ROW_TILE
    per = NEAR_PIECE // ROW_TILE
    row = pl.BlockSpec((ROW_TILE, width), lambda i, *_: (jnp.minimum(i, tiles - 1), 0))
    lower = pl.BlockSpec((ROW_TILE, width), lambda i, *_: (jnp.minimum(i, per - 1), 0))
    upper = pl.BlockSpec((ROW_TILE, width), lambda i, *_: (jnp.clip(i - per, 0, per - 1), 0))
    anyspec = pl.BlockSpec(memory_space=pl.ANY)
    return pl.pallas_call(
        norm_kernel,
        grid_spec=pltpu.PrefetchScalarGridSpec(
            num_scalar_prefetch=2, grid=(tiles + 1,),
            in_specs=[lower, upper] * 2 + [anyspec] * 4 + [row, row, pl.BlockSpec((1, width), lambda i, *_: (0, 0))],
            out_specs=[row, row, pl.BlockSpec((ROW_TILE, width), lambda i, *_: (i, 0))],
            scratch_shapes=[
                pltpu.VMEM((FAR_CAP + 8, width), jnp.float32),
                pltpu.VMEM((ROW_TILE, width), jnp.float32),
                pltpu.VMEM((16, width), jnp.float32),
                pltpu.SemaphoreType.DMA((4,)),
            ],
        ),
        out_shape=(jax.ShapeDtypeStruct((rows, width), jnp.bfloat16),
                   jax.ShapeDtypeStruct((rows, width), jnp.bfloat16),
                   jax.ShapeDtypeStruct((rows + 8, width), jnp.float32)),
        compiler_params=pltpu.CompilerParams(vmem_limit_bytes=60 * 2**20),
        name="assemble_norm",
    )(core, slots, *own, *theirs, *far, dyn, dyr, w)


def solution(mesh):
    def plan(all_ids, rows):
        n = all_ids.shape[0]
        dp, tp = lax.axis_index("dp"), lax.axis_index("tp")
        me, core = tp * 4 + dp, tp % 2
        keys = lax.sort(all_ids * n + lax.iota(jnp.int32, n), is_stable=False)
        ids, idx = keys >> 13, keys & (n - 1)
        differs = ids[1:] != ids[:-1]
        one = jnp.ones((1,), jnp.int32)
        first = jnp.concatenate([one, differs.astype(jnp.int32)])
        slot = jnp.cumsum(first) - 1
        edges = jnp.arange(NDEV + 1, dtype=jnp.int32) * OWN_ROWS
        starts = jnp.sum(jnp.where(ids[None, :] < edges[:, None], first[None, :], 0), axis=1)
        caps = jnp.array(CAPS, jnp.int32)
        overflow = jnp.any(starts[1:] - starts[:-1] > caps)
        chip = idx >> 10
        fresh = jnp.concatenate([one, (differs | (chip[1:] != chip[:-1])).astype(jnp.int32)])
        far = jnp.where((ids >> 15) != (chip & 1), fresh, 0)
        per_chip = jnp.sum(jnp.where(chip[None, :] == jnp.arange(8, dtype=jnp.int32)[:, None], far[None, :], 0), axis=1)
        overflow = overflow | jnp.any(per_chip > FAR_CAP)
        owner = ids // OWN_ROWS
        hit = owner[None, :] == jnp.arange(NDEV, dtype=jnp.int32)[:, None]
        offset = jnp.sum(jnp.where(hit, starts[:-1][:, None], 0), axis=0)
        hbase = jnp.sum(jnp.where(hit, jnp.array(HBASE, jnp.int32)[:, None], 0), axis=0)
        local_slot = slot - offset
        pos = jnp.minimum(hbase + local_slot // 2, HTOT - 1)
        mine = local_slot % 2 == core
        src = (idx // 512) * rows + idx % 512
        work = lax.sort(jnp.where(mine, 0, 1 << 26) + src * 4096 + pos, is_stable=False)
        count = jnp.sum(mine.astype(jnp.int32)).reshape(1)
        uniq = lax.sort(jnp.where(first == 1, ids, 1 << 20), is_stable=False)
        uniq = jnp.concatenate([uniq, jnp.full((CAPMAX,), 1 << 20, jnp.int32)])
        my_start = jnp.sum(jnp.where(jnp.arange(NDEV) == me, starts[:-1], 0))
        my_ids = lax.dynamic_slice(uniq, (my_start,), (CAPMAX,))
        tiles = me * OWN_ROWS + jnp.arange(OWN_ROWS // TILE + 1, dtype=jnp.int32) * TILE
        bounds = jnp.sum(jnp.where(ids[None, :] < tiles[:, None], first[None, :], 0), axis=1) - my_start
        my_half = jnp.sum(jnp.where(jnp.arange(NDEV) == me, jnp.array(HALF, jnp.int32), 0))
        bounds = jnp.concatenate([bounds, my_half[None], (me * OWN_ROWS)[None]]).astype(jnp.int32)
        return overflow, work, count, my_ids, bounds

    def far_lists(ids):
        n = ids.shape[1]
        pos = lax.iota(jnp.int32, n)
        same = ids[:, :, None] == ids[:, None, :]
        lead = jnp.min(jnp.where(same, pos[None, :, None], n), axis=1)
        far = (ids >> 15) != jnp.arange(2, dtype=jnp.int32)[:, None]
        first = (lead == pos[None]) & far
        slot = jnp.sum(jnp.where(first[:, :, None] & (pos[None, :, None] < lead[:, None, :]), 1, 0), axis=1)
        slots = lax.iota(jnp.int32, FAR_CAP)
        at = first[:, :, None] & (slot[:, :, None] == slots[None, None, :])
        listed = jnp.max(jnp.where(at, ids[:, :, None], -1), axis=1)
        return listed, jnp.where(far, jnp.minimum(slot, FAR_CAP - 1), FAR_CAP)

    def local_step(tokens, emb_table, w_norm, dy_norm, dy_resid):
        shard_rows, model_dim = emb_table.shape
        scale_float = jnp.asarray(math.sqrt(model_dim), jnp.bfloat16).astype(jnp.float32)
        scale_py = float(np.array(math.sqrt(model_dim)).astype(jnp.dtype(jnp.bfloat16)))
        dp, tp = lax.axis_index("dp"), lax.axis_index("tp")
        x, c = tp // 2, tp % 2
        seq = tokens.shape[1]
        part = seq // 4
        swap_core = [(t, t ^ 1) for t in range(4)]
        swap_x = [(t, t ^ 2) for t in range(4)]

        def raw(ids):
            ids = ids - tp * shard_rows
            owned = (ids >= 0) & (ids < shard_rows)
            return jnp.take(emb_table, jnp.where(owned, ids, 0), axis=0, mode="clip"), owned[:, None]

        def scaled(got, owned):
            return jnp.where(owned, got.astype(jnp.float32) * scale_float, 0.0)

        def fetch(ids):
            return scaled(*raw(ids))

        def positions(toks, px, pc):
            return lax.dynamic_slice(toks, ((px * 2 + pc) * part,), (part,))

        listed, slots = far_lists(tokens.reshape(2, seq // 2))
        my_list = jnp.where(x == 0, listed[1], listed[0])
        my_slots = lax.dynamic_slice(slots.reshape(-1), (tp * part,), (part,))
        half, at = FAR_CAP // 2, 0
        got, toks = [], tokens[0]
        for n in FAR_CHUNKS:
            theirs = lax.dynamic_slice(my_list, ((1 - c) * half + at,), (n,))
            mine = lax.dynamic_slice(my_list, (c * half + at,), (n,))
            at += n
            pair, mask = lax.optimization_barrier(raw(jnp.concatenate([theirs, mine])))
            both = lax.ppermute(scaled(pair[:n], mask[:n]), "tp", swap_core) + scaled(pair[n:], mask[n:])
            both, my_list, toks = lax.optimization_barrier((both, my_list, toks))
            got.append(lax.ppermute(both, "tp", swap_x))
        relayed = [lax.ppermute(r, "tp", swap_core) for r in got]
        near_own, near_theirs = [], []
        for k in range(part // NEAR_PIECE):
            theirs = fetch(positions(toks, x, 1 - c)[k * NEAR_PIECE:(k + 1) * NEAR_PIECE])
            near_theirs.append(lax.ppermute(theirs, "tp", swap_core))
        all_ids = lax.all_gather(toks[None], "dp", axis=0, tiled=True).reshape(-1)
        for k in range(part // NEAR_PIECE):
            near_own.append(fetch(positions(toks, x, c)[k * NEAR_PIECE:(k + 1) * NEAR_PIECE]))
        near_own = lax.optimization_barrier(near_own)
        rows = part + 8
        overflow, work, count, my_ids, bounds = plan(all_ids, rows)

        def dense_forward(near_own, near_theirs, toks):
            near = jnp.concatenate(near_own, axis=0) + jnp.concatenate(near_theirs, axis=0)
            far = lax.ppermute(fetch(positions(toks, 1 - x, 1 - c)), "tp", swap_core) + fetch(positions(toks, 1 - x, c))
            x_emb = (near + lax.ppermute(far, "tp", swap_x)).astype(jnp.bfloat16)
            x_float = x_emb.astype(jnp.float32)
            inv_rms = lax.rsqrt(jnp.mean(x_float * x_float, axis=-1, keepdims=True) + NORM_EPS)
            x_hat = x_float * inv_rms
            norm_gain = 1.0 + w_norm
            y_norm = (x_hat * norm_gain).astype(jnp.bfloat16)
            dy_float = dy_norm[0].astype(jnp.float32)
            dx_hat = dy_float * norm_gain
            tok_grad = dy_resid[0].astype(jnp.float32) + inv_rms * (dx_hat - x_hat * jnp.mean(dx_hat * x_hat, axis=-1, keepdims=True))
            w_part = jnp.sum(dy_float * x_hat, axis=0)
            return x_emb, y_norm, jnp.concatenate([tok_grad, jnp.pad(w_part[None], ((0, 7), (0, 0)))], axis=0)

        def sparse_forward(near_own, near_theirs, toks):
            core = c.astype(jnp.int32).reshape(1)
            return tuple(norm(core, my_slots, near_own, near_theirs, got + relayed, dy_norm[0], dy_resid[0], w_norm[None]))

        x_emb, y_norm, g_ext = lax.cond(overflow, dense_forward, sparse_forward, near_own, near_theirs, toks)

        cols = exchange_columns(g_ext)
        acc = sum_duplicates(work, count, cols, part)
        owned, w_rows = send_to_owners(acc)

        def dense_backward(g_ext, owned):
            g = g_ext[:part]
            ids = tokens[0] - tp * shard_rows
            seq_grad = jnp.zeros((seq, model_dim), jnp.float32)
            for s in range(4):
                block = g if s == 0 else lax.ppermute(g, "tp", [(t, (t + s) % 4) for t in range(4)])
                seq_grad = lax.dynamic_update_slice(seq_grad, block, ((tp + 4 - s) % 4 * part, 0))
            drop_ids = jnp.where((ids >= 0) & (ids < shard_rows), ids, shard_rows)
            shard_grad = jax.ops.segment_sum(seq_grad, drop_ids, num_segments=shard_rows, mode="drop") * scale_float
            total = lax.dynamic_slice(shard_grad, (dp * OWN_ROWS, 0), (OWN_ROWS, model_dim))
            for s in range(1, 4):
                block = lax.dynamic_slice(shard_grad, ((dp + s) % 4 * OWN_ROWS, 0), (OWN_ROWS, model_dim))
                total = total + lax.ppermute(block, "dp", [(d, (d + s) % 4) for d in range(4)])
            return total

        def sparse_backward(g_ext, owned):
            return expand(bounds, my_ids, owned, scale_py)

        emb_grad = lax.cond(overflow, dense_backward, sparse_backward, g_ext, owned)
        return x_emb[None], y_norm[None], emb_grad, w_rows[0]

    act_spec = P("dp", "tp", None)
    return jax.shard_map(local_step, mesh=mesh, in_specs=(P("dp", None), P("tp", None), P(None), act_spec, act_spec), out_specs=(act_spec, act_spec, P(("tp", "dp"), None), P(None)), check_vma=False)
```
